32 devices in a mesh: cluster: 4 (over x, core), leaf: 8 (over z, y).
Axes of the slice: x: 2, y: 2, z: 4, core: 2. Of those that a mesh axis runs over, the one named last changes fastest.
Arguments:
- probes: float32 [32768, 512], P(('cluster', 'leaf')), may hold values from -6 to 6
- dense_leaf: float32 [32768, 1024], P(('cluster', 'leaf')), may hold values from -0.1875 to 0.1875
- leaf_basis: float32 [32768, 128], P(('cluster', 'leaf')), may hold values from -0.1875 to 0.1875
- sibling_cores: float32 [32, 8, 128, 128], P(('cluster', 'leaf')), may hold values from -0.5 to 0.5
- transfer: float32 [32, 128, 128], P(('cluster', 'leaf')), may hold values from -0.5 to 0.5
- cluster_cores: float32 [4, 4, 128, 128], P('cluster'), may hold values from -0.1875 to 0.1875
Outputs:
- product: float32 [32768, 512], P(('cluster', 'leaf'))
The draws below stay inside these ranges and needn't reach their ends.
All inputs are finite; a program needn't handle non-finite values.
Results may differ from the reference program's by a relative error of at most 0.00005.
Values sent between devices are 32-bit elements; how exact they have to be, the bound alone decides.
No kernel may reach another device: no remote copies, remote signals or barrier semaphores. Data moves between devices by JAX's collectives and lax.ppermute only.
A program may use at most 128 MiB of HBM per device.

```python
import jax
import jax.numpy as jnp
from jax import lax

LEAF = 1024
R = 128
R2 = 128
P_SIZE = 512
LEAVES = 32
ORDER = 32768
N_CLUSTER = 4
N_LEAF = 8


def levels(own_key, shape, cuts, least, largest):
    level = 1.0
    for position, blocks in cuts:
        steps = jax.random.uniform(jax.random.fold_in(jax.random.fold_in(own_key, 6), position), (blocks,), jnp.float32, least / len(cuts), largest / len(cuts))
        level = level * jnp.repeat(jnp.exp(steps), shape[position] // blocks).reshape((-1,) + (1,) * (len(shape) - 1 - position))
    return level


def scatter_about(key, extent, deviation, most, split=(), held_as=jnp.bfloat16):
    entries = jax.random.normal(key, extent, jnp.float32) * deviation
    if len(split) > 0:
        entries = levels(key, extent, split, -0.22, 0.18) * entries
    return jnp.clip(entries, min=-most, max=most).astype(held_as)


def setup_inputs(seed: int = 0) -> dict:
    arg_keys = jax.random.split(jax.random.key(seed), 7)
    return {
        "probes": scatter_about(arg_keys[0], (ORDER, P_SIZE), 1.0, 6.0, ((0, 32),), jnp.float32),
        "dense_leaf": scatter_about(arg_keys[1], (ORDER, LEAF), LEAF ** -0.5, 0.1875, ((0, 32),), jnp.float32),
        "leaf_basis": scatter_about(arg_keys[2], (ORDER, R), LEAF ** -0.5, 0.1875, ((0, 32),), jnp.float32),
        "sibling_cores": scatter_about(arg_keys[3], (LEAVES, N_LEAF, R, R), (R * N_LEAF // 8) ** -0.5, 0.5, ((0, 32),), jnp.float32),
        "transfer": scatter_about(arg_keys[4], (LEAVES, R, R2), R ** -0.5, 0.5, ((0, 32),), jnp.float32),
        "cluster_cores": scatter_about(arg_keys[5], (N_CLUSTER, N_CLUSTER, R2, R2), (R2 * N_CLUSTER * N_LEAF // 4) ** -0.5, 0.1875, ((0, 4),), jnp.float32),
    }


HI = lax.Precision.HIGHEST


def reference(probes, dense_leaf, leaf_basis, sibling_cores, transfer, cluster_cores):
    nclu = N_CLUSTER
    nleaf = N_LEAF
    xl = probes.reshape(nclu, nleaf, LEAF, P_SIZE)
    dl = dense_leaf.reshape(nclu, nleaf, LEAF, LEAF)
    ul = leaf_basis.reshape(nclu, nleaf, LEAF, R)
    near = jnp.einsum('cnab,cnbp->cnap', dl, xl, precision=HI) + jnp.einsum('cnba,cnbp->cnap', dl, xl, precision=HI)
    coef = jnp.einsum('cnar,cnap->cnrp', ul, xl, precision=HI)
    keep = (1.0 - jnp.eye(nleaf, dtype=jnp.float32))[None, :, :, None, None]
    cores = sibling_cores.reshape(nclu, nleaf, nleaf, R, R) * keep
    sib = jnp.einsum('cijab,cjbp->ciap', cores, coef, precision=HI) + jnp.einsum('cjiba,cjbp->ciap', cores, coef, precision=HI)
    el = transfer.reshape(nclu, nleaf, R, R2)
    g = jnp.sum(jnp.einsum('cnrs,cnrp->cnsp', el, coef, precision=HI), axis=1)
    bkeep = (1.0 - jnp.eye(nclu, dtype=jnp.float32))[:, :, None, None]
    bm = cluster_cores * bkeep
    h = jnp.einsum('cdab,dbp->cap', bm, g, precision=HI) + jnp.einsum('dcba,dbp->cap', bm, g, precision=HI)
    total = sib + jnp.einsum('cnrs,csp->cnrp', el, h, precision=HI)
    out = near + jnp.einsum('cnar,cnrp->cnap', ul, total, precision=HI)
    return out.reshape(nclu * nleaf * LEAF, P_SIZE)
```

```python
import jax
import jax.numpy as jnp
from jax import lax
from jax.sharding import PartitionSpec as P

HI = lax.Precision.HIGH


def dot(a, b, da, db):
    return lax.dot_general(a, b, (((da,), (db,)), ((), ())), precision=HI)


def local(probes, dense_leaf, leaf_basis, sibling_cores, transfer, cluster_cores):
    n_leaf = lax.axis_size("leaf")
    n_clu = lax.axis_size("cluster")
    half = n_leaf // 2
    pairs_x = n_clu // 2
    own = lax.axis_index("leaf")
    cown = lax.axis_index("cluster")
    z = own // 2
    y = own % 2
    core = cown % 2
    xpos = cown // 2
    cores = sibling_cores[0]
    trans = transfer[0]
    outer = cluster_cores[0]
    rank = trans.shape[0]
    rank2 = trans.shape[1]
    cols = probes.shape[1]
    piece = cols // n_leaf

    def swap(v):
        return lax.ppermute(v, "leaf", [(i, i ^ 1) for i in range(n_leaf)])

    def shift(v, s):
        return lax.ppermute(v, "leaf", [(i, ((i // 2 + s) % half) * 2 + i % 2) for i in range(n_leaf)])

    coef = dot(leaf_basis, probes, 0, 0)
    grid = cores.reshape(half, 2, rank, rank)

    got_cores = {}
    for s in range(1, half):
        target = (z + s) % half
        got_cores[s] = shift(lax.dynamic_index_in_dim(grid, target, 0, keepdims=False), s)

    gt = dot(coef, trans, 0, 0)
    gt = gt.reshape(2, cols // 2, rank2)
    keep = lax.dynamic_index_in_dim(gt, y, 0, keepdims=False)
    give = lax.dynamic_index_in_dim(gt, 1 - y, 0, keepdims=False)
    gpair = (keep + swap(give)).reshape(half, piece, rank2)

    gd = lax.dynamic_index_in_dim(gpair, z, 0, keepdims=False)
    for s in range(1, half):
        gd = gd + shift(lax.dynamic_index_in_dim(gpair, (z + s) % half, 0, keepdims=False), s)

    got_coef = {0: coef}
    for s in range(1, half):
        got_coef[s] = shift(coef, s)

    ckeep = (jnp.arange(n_clu, dtype=jnp.int32) != cown).astype(jnp.float32)[:, None, None]
    masked = outer * ckeep
    turned = jnp.stack([dot(gd, masked[c], 1, 0) for c in range(n_clu)])
    turned = turned.reshape(pairs_x, 2, piece, rank2)
    mine = lax.dynamic_index_in_dim(turned, core, 1, keepdims=False)
    theirs = lax.dynamic_index_in_dim(turned, 1 - core, 1, keepdims=False)
    buddy = lax.ppermute(
        jnp.concatenate([gd[None], theirs]), "cluster", [(i, i ^ 1) for i in range(n_clu)]
    )
    gboth = jnp.stack([gd, buddy[0]])
    sums = mine + buddy[1:]
    ht = lax.dynamic_index_in_dim(sums, xpos, 0, keepdims=False)
    pair_blocks = masked.reshape(pairs_x, 2, rank2, rank2)

    def front(both, xi):
        blocks = lax.dynamic_index_in_dim(pair_blocks, xi, 0, keepdims=False)
        same = lax.dynamic_index_in_dim(blocks, core, 0, keepdims=False)
        other = lax.dynamic_index_in_dim(blocks, 1 - core, 0, keepdims=False)
        return dot(both[0], same, 1, 1) + dot(both[1], other, 1, 1)

    ht = ht + front(gboth, xpos)
    for s in range(1, pairs_x):
        target = (xpos + s) % pairs_x
        sent = jnp.concatenate([gboth, lax.dynamic_index_in_dim(sums, target, 0)])
        back = lax.ppermute(
            sent, "cluster", [(i, ((i // 2 + s) % pairs_x) * 2 + i % 2) for i in range(n_clu)]
        )
        ht = ht + back[2] + front(back, (xpos - s) % pairs_x)

    hline = jnp.zeros((half, piece, rank2), jnp.float32)
    hline = lax.dynamic_update_index_in_dim(hline, ht, z, 0)
    for s in range(1, half):
        hline = lax.dynamic_update_index_in_dim(hline, shift(ht, s), (z - s) % half, 0)
    hline = hline.reshape(half * piece, rank2)

    rows_other = lax.dynamic_index_in_dim(grid, 1 - y, 1, keepdims=False)
    rows_own = lax.dynamic_index_in_dim(grid, y, 1, keepdims=False)
    from_pair = swap(jnp.concatenate([rows_other, trans[None]]))
    rows_pair = from_pair[:half]
    trans_pair = from_pair[half]

    part_own = None
    part_pair = None
    for s in range(half):
        src = (z - s) % half
        a_pair = lax.dynamic_index_in_dim(rows_pair, src, 0, keepdims=False)
        if s == 0:
            turned_pair = lax.dynamic_index_in_dim(
                lax.dynamic_index_in_dim(grid, z, 0, keepdims=False), 1 - y, 0, keepdims=False
            )
            part_pair = dot(a_pair + turned_pair.T, got_coef[0], 1, 0)
        else:
            a_own = lax.dynamic_index_in_dim(rows_own, src, 0, keepdims=False)
            to_own = lax.dynamic_index_in_dim(got_cores[s], y, 0, keepdims=False)
            to_pair = lax.dynamic_index_in_dim(got_cores[s], 1 - y, 0, keepdims=False)
            p = dot(a_own + to_own.T, got_coef[s], 1, 0)
            part_own = p if part_own is None else part_own + p
            part_pair = part_pair + dot(a_pair + to_pair.T, got_coef[s], 1, 0)

    low_own = dot(trans, hline, 1, 1)
    low_pair = dot(trans_pair, hline, 1, 1)

    def place(v):
        wide = jnp.zeros((rank, 2, cols // 2), jnp.float32)
        return lax.dynamic_update_index_in_dim(wide, v, y, 1).reshape(rank, cols)

    if part_own is None:
        part_own = jnp.zeros((rank, cols), jnp.float32)
    total = part_own + place(low_own) + swap(part_pair + place(low_pair))
    near = dot(dense_leaf + dense_leaf.T, probes, 1, 0)
    return near + dot(leaf_basis, total, 1, 0)


def solution(mesh):
    return jax.shard_map(
        local,
        mesh=mesh,
        in_specs=(
            P(("cluster", "leaf"), None),
            P(("cluster", "leaf"), None),
            P(("cluster", "leaf"), None),
            P(("cluster", "leaf"), None, None, None),
            P(("cluster", "leaf"), None, None),
            P("cluster", None, None, None),
        ),
        out_specs=P(("cluster", "leaf"), None),
        check_vma=False,
    )
```
